32 devices in a mesh: ctx: 8 (over z, core), tp: 4 (over y, x).
Axes of the slice: x: 2, y: 2, z: 4, core: 2. Of those that a mesh axis runs over, the one named last changes fastest.
Arguments:
- act_codes: bfloat16 [2048, 4096], P(('ctx', 'tp')), may hold values from -6 to 6
- scale_exps: int32 [2048, 32], P(('ctx', 'tp')), may hold values from -2 to 2
- weight: bfloat16 [4096, 6144], P(None, 'tp'), may hold values from -0.09375 to 0.09375
- grad_out: bfloat16 [2048, 6144], P('ctx', 'tp'), may hold values from -6 to 6
Outputs:
- grad_input: bfloat16 [2048, 4096], P(('ctx', 'tp'))
- grad_weight: float32 [4096, 6144], P('ctx', 'tp')
The draws below stay inside these ranges and needn't reach their ends.
All inputs are finite; a program needn't handle non-finite values.
Results may differ from the reference program's by a relative error of at most 0.023.
Values may be sent and summed in bfloat16 or wider, within the bound.
No kernel may reach another device: no remote copies, remote signals or barrier semaphores. Data moves between devices by JAX's collectives and lax.ppermute only.
A program may use at most 64 MiB of HBM per device.

```python
import jax
import jax.numpy as jnp
from jax import lax

D = 4096
BLOCK = 128
QKVW = 6144
TOKENS = 2048
N_TP = 4


def plant(array, own_key, least, high):
    place = [jax.random.randint(jax.random.fold_in(own_key, axis), (), 0, length) for axis, length in enumerate(array.shape)]
    longest = array.shape.index(max(array.shape))
    neighbour = place[:longest] + [(place[longest] + 1) % array.shape[longest]] + place[longest + 1:]
    return array.at[tuple(place)].set(least).at[tuple(neighbour)].set(high)


def strengthened(array, own_key, source, target, parts, factor):
    owner, partner = [(jnp.arange(array.shape[axis_at]) // (array.shape[axis_at] // parts)).reshape([-1 if axis == axis_at else 1 for axis in range(array.ndim)]) for axis_at in (source, target)]
    chosen = jax.random.permutation(own_key, parts)[partner]
    strong = (owner == chosen) | (owner == (partner + parts // 2) % parts)
    return jnp.where(strong, factor * array, array)


def levels(stream_key, shape, shards, low, top_value):
    loudness, own = 1.0, jax.random.fold_in(stream_key, 6)
    for position, parts in shards:
        steps = jnp.exp(jax.random.uniform(jax.random.fold_in(own, position), (parts,), jnp.float32, low / len(shards), top_value / len(shards)))
        loudness = loudness * jnp.repeat(steps, shape[position] // parts).reshape([-1 if axis == position else 1 for axis in range(len(shape))])
    return loudness


def gaussian(own_key, dims, deviation, reach, cuts=(), kind=jnp.bfloat16):
    values = jax.random.normal(own_key, dims, jnp.float32) * deviation
    if len(cuts) > 0:
        values = levels(own_key, dims, cuts, -0.22, 0.18) * values
    return jnp.clip(values, min=-reach, max=reach).astype(kind)


def noise_with(stream_key, extent, scale, reach, pieces, heavy, held_as=jnp.bfloat16):
    drawn = scale * jax.random.normal(stream_key, extent, jnp.float32)
    if pieces:
        drawn = drawn * levels(stream_key, extent, pieces, -0.22, 0.18)
    return jnp.clip(strengthened(drawn, jax.random.fold_in(stream_key, 3), *heavy), -reach, reach).astype(held_as)


def setup_inputs(seed: int = 0) -> dict:
    key_list = jax.random.split(jax.random.key(seed), 5)
    act_codes = noise_with(key_list[0], (TOKENS, D), 1.0, 6.0, ((0, 32),), (0, 1, 32, 2.75))
    scale_exps = plant(jax.random.randint(key_list[1], (TOKENS, D // BLOCK), -2, 3), jax.random.fold_in(key_list[1], 1), -2, 2).astype(jnp.int32)
    weight = gaussian(key_list[2], (D, QKVW), D ** -0.5, 0.09375, ((1, 4),))
    grad_out = noise_with(key_list[3], (TOKENS, QKVW), 1.0, 6.0, ((0, 8), (1, 4)), (1, 0, 8, 2.0))
    return {"act_codes": act_codes, "scale_exps": scale_exps, "weight": weight, "grad_out": grad_out}


def dequantize(act_codes, scale_exps):
    tok_rows = act_codes.shape[0]
    scales = jnp.exp2(scale_exps.astype(jnp.float32))
    blocked = act_codes.astype(jnp.float32).reshape(tok_rows, D // BLOCK, BLOCK) * scales[:, :, None]
    return blocked.reshape(tok_rows, D).astype(jnp.bfloat16)

def reference(act_codes, scale_exps, weight, grad_out):
    acts = dequantize(act_codes, scale_exps)
    grad_weight = jnp.dot(acts.T, grad_out, preferred_element_type=jnp.float32)
    grad_weight = grad_weight * lax.rsqrt(jnp.float32(TOKENS))
    width = QKVW // N_TP

    def add_block(total, index):
        offset = (index * width).astype(jnp.int32)
        grads = lax.dynamic_slice_in_dim(grad_out, offset, width, 1)
        weights = lax.dynamic_slice_in_dim(weight, offset, width, 1)
        part = lax.dot_general(grads, weights, (((1,), (1,)), ((), ())), preferred_element_type=jnp.float32)
        part = lax.optimization_barrier(part.astype(jnp.bfloat16))
        return (total + part.astype(jnp.float32), None)
    total, unused = lax.scan(add_block, jnp.zeros((TOKENS, D), jnp.float32), jnp.arange(N_TP, dtype=jnp.int32))
    return (total.astype(jnp.bfloat16), grad_weight)
```

```python
import jax
import jax.numpy as jnp
import numpy as np
from jax import lax
from jax.sharding import PartitionSpec as P


def dequantize(codes, exponents, block):
    tok_rows, width = codes.shape
    scales = jnp.exp2(exponents.astype(jnp.float32))
    blocked = (
        codes.astype(jnp.float32).reshape(tok_rows, width // block, block) * scales[:, :, None]
    )
    return blocked.reshape(tok_rows, width).astype(jnp.bfloat16)


def ring_order(length):
    return list(range(0, length, 2)) + list(range(length - 1 - (length % 2), 0, -2))


def tdot(a, b):
    return lax.dot_general(a, b, (((0,), (0,)), ((), ())), preferred_element_type=jnp.float32)


def body(act_codes, scale_exps, weight, grad_out):
    width = act_codes.shape[1]
    block = width // scale_exps.shape[1]
    n_ctx, n_tp = lax.axis_size("ctx"), lax.axis_size("tp")
    chips = n_ctx // 2
    ctx, tp = lax.axis_index("ctx"), lax.axis_index("tp")
    chip, core = ctx // 2, ctx % 2
    rows = act_codes.shape[0]
    out_rows = width // n_ctx
    order = ring_order(chips)
    place = {k: i for i, k in enumerate(order)}

    swap = [(i, i ^ 1) for i in range(n_ctx)]

    def shift(step):
        return [
            (2 * order[i] + c, 2 * order[(i + step) % chips] + c)
            for i in range(chips)
            for c in range(2)
        ]

    def peers(j):
        return [(i, i ^ j) for i in range(n_tp)]

    ring = [grad_out]
    for _ in range(chips - 1):
        ring.append(lax.ppermute(ring[-1], "ctx", shift(1)))
    partner = [lax.ppermute(g, "ctx", swap) for g in ring]

    acts = dequantize(act_codes, scale_exps, block).reshape(rows, chips, 2, out_rows)
    acts = acts.transpose(2, 1, 0, 3)
    mine = jnp.where(core == 0, acts[0], acts[1])
    theirs = jnp.where(core == 0, acts[1], acts[0])
    other = lax.ppermute(theirs, "ctx", swap)
    both = jnp.stack([mine, other], axis=1)
    pieces = []
    for step in range(chips):
        table = np.array([order[(place[k] + step) % chips] for k in range(chips)], np.int32)
        sent = lax.dynamic_index_in_dim(both, jnp.asarray(table)[chip], 0, keepdims=False)
        pieces.append(lax.ppermute(sent, "ctx", shift(step)) if step else sent)
    pieces = jnp.stack(pieces)
    gathered = jnp.zeros((chips, 2, n_tp, rows, out_rows), jnp.bfloat16)
    for j in range(n_tp):
        got = lax.ppermute(pieces, "tp", peers(j)) if j else pieces
        gathered = lax.dynamic_update_slice(gathered, got[:, :, None], (0, 0, tp ^ j, 0, 0))
    gathered = gathered.reshape(chips, 2, n_tp * rows, out_rows)

    part = lax.dot_general(
        grad_out, weight, (((1,), (1,)), ((), ())), preferred_element_type=jnp.float32
    ).astype(jnp.bfloat16)
    total = None
    for j in range(n_tp):
        sent = lax.dynamic_slice_in_dim(part, (tp ^ j) * rows, rows, 0)
        got = (lax.ppermute(sent, "tp", peers(j)) if j else sent).astype(jnp.float32)
        total = got if total is None else total + got
    grad_input = total.astype(jnp.bfloat16)

    tokens_all = grad_out.shape[0] * n_ctx
    summed = None
    for step in range(chips):
        for source, side in ((ring[step], 0), (partner[step], 1)):
            term = tdot(gathered[step, side], source)
            summed = term if summed is None else summed + term
    grad_weight = summed * lax.rsqrt(jnp.float32(tokens_all))
    return (grad_input, grad_weight)


def solution(mesh):
    placed = (P(("ctx", "tp"), None), P(("ctx", "tp"), None), P(None, "tp"), P("ctx", "tp"))
    return jax.shard_map(
        body,
        mesh=mesh,
        in_specs=placed,
        out_specs=(P(("ctx", "tp"), None), P("ctx", "tp")),
        check_vma=False,
    )
```

```python
import functools

import jax
import jax.numpy as jnp
from jax import lax
from jax.experimental import pallas as pl
from jax.experimental.pallas import tpu as pltpu
from jax.sharding import PartitionSpec as P

VMEM = pl.BlockSpec(memory_space=pltpu.VMEM)


def ring_order(length):
    return list(range(0, length, 2)) + list(range(length - 1 - (length % 2), 0, -2))


def prepare_kernel(order, block, codes_ref, exps_ref, *out_refs):
    chips = len(order)
    wide = out_refs[0].shape[-1]
    per = wide // block
    chip = lax.axis_index("ctx") // 2
    exps = exps_ref[...].astype(jnp.float32).T
    for step, out_ref in enumerate(out_refs):
        dest = jnp.int32(0)
        for i in range(chips):
            dest = dest + jnp.where(chip == order[i], order[(i + step) % chips], 0)
        chosen = jnp.zeros((exps.shape[0], per), jnp.float32)
        for k in range(chips):
            chosen = jnp.where(dest == k, exps[:, per * k : per * (k + 1)], chosen)
        scales = jnp.exp2(chosen)
        for j in range(per):
            column = pl.multiple_of(dest * wide + j * block, block)
            codes = codes_ref[:, pl.ds(column, block)].astype(jnp.float32)
            out_ref[:, j * block : (j + 1) * block] = (codes * scales[:, j : j + 1]).astype(
                jnp.bfloat16
            )


def prepare(codes, exponents, order):
    rows, width = codes.shape
    chips = len(order)
    out = jax.ShapeDtypeStruct((rows, width // chips), jnp.bfloat16)
    return pl.pallas_call(
        functools.partial(prepare_kernel, order, width // exponents.shape[1]),
        out_shape=[out] * chips,
        in_specs=[VMEM] * 2,
        out_specs=[VMEM] * chips,
        cost_estimate=pl.CostEstimate(
            flops=2 * rows * width, bytes_accessed=4 * rows * width, transcendentals=0
        ),
    )(codes, exponents.T)


def tdot(a, b):
    return lax.dot_general(a, b, (((0,), (0,)), ((), ())), preferred_element_type=jnp.float32)


def added(terms):
    return sum(t.astype(jnp.float32) for t in terms).astype(jnp.bfloat16)


def body(act_codes, scale_exps, weight, grad_out):
    width = act_codes.shape[1]
    n_ctx, n_tp = lax.axis_size("ctx"), lax.axis_size("tp")
    chips = n_ctx // 2
    tp = lax.axis_index("tp")
    rows = act_codes.shape[0]
    tokens = grad_out.shape[0]
    out_rows = width // n_ctx
    core = lax.axis_index("ctx") % 2
    order = ring_order(chips)
    half = tokens // 2

    swap = [(i, i ^ 1) for i in range(n_ctx)]

    def shift(step):
        return [
            (2 * order[i] + c, 2 * order[(i + step) % chips] + c)
            for i in range(chips)
            for c in range(2)
        ]

    def peers(j):
        return [(i, i ^ j) for i in range(n_tp)]

    every = jnp.zeros((chips * tokens, grad_out.shape[1]), jnp.bfloat16)
    every = lax.dynamic_update_slice(every, grad_out, (0, 0))
    moving = lax.ppermute(grad_out, "ctx", shift(1))
    every = lax.dynamic_update_slice(every, moving, (tokens, 0))
    moving = [moving[:half], moving[half:]]
    for step in range(2, chips):
        for h in range(2):
            moving[h] = lax.ppermute(moving[h], "ctx", shift(1))
            if step < chips - 1 or h == 0:
                every = lax.dynamic_update_slice(every, moving[h], (step * tokens + h * half, 0))

    pieces = list(prepare(act_codes, scale_exps, order))
    for step in range(1, chips):
        pieces[step] = lax.ppermute(pieces[step], "ctx", shift(step))
    pieces = jnp.stack(pieces)
    got = {0: pieces}
    if n_tp == 4:
        for j in (1, 2):
            got[j] = lax.ppermute(pieces, "tp", peers(j))
        middle = chips // 2
        first = lax.ppermute(got[1][:middle], "tp", peers(2))
        second = lax.ppermute(got[2][middle:], "tp", peers(1))
    else:
        for j in range(1, n_tp):
            got[j] = lax.ppermute(pieces, "tp", peers(j))
    if n_tp == 4:
        got[3] = None
    sides = []
    for side in range(2):
        acts = jnp.zeros((chips, n_tp, rows, out_rows), jnp.bfloat16)
        for j, part in got.items():
            blocks = [(0, part)] if part is not None else [(0, first), (middle, second)]
            for at, block in blocks:
                block = jnp.where(core == side, block[..., :out_rows], block[..., out_rows:])
                acts = lax.dynamic_update_slice(acts, block[:, None], (at, tp ^ j, 0, 0))
        sides.append(acts.reshape(chips * tokens, out_rows))

    outs = []
    span = width // 2
    bits = [1 << b for b in range(n_tp.bit_length() - 1)]
    for h in range(2):
        part = lax.dot_general(
            grad_out,
            lax.slice_in_dim(weight, h * span, (h + 1) * span),
            (((1,), (1,)), ((), ())),
            preferred_element_type=jnp.float32,
        ).astype(jnp.bfloat16)
        held = {j: [lax.dynamic_slice_in_dim(part, (tp ^ j) * rows, rows, 0)] for j in range(n_tp)}
        for bit in bits if h == 0 else bits[::-1]:
            leaving = [j for j in held if j & bit]
            sent = jnp.stack([added(held.pop(j)) for j in leaving])
            sent = lax.ppermute(sent, "tp", peers(bit))
            for i, j in enumerate(leaving):
                held[j ^ bit].append(sent[i])
        outs.append(added(held[0]))
    grad_input = jnp.concatenate(outs, axis=1)

    scale = lax.rsqrt(jnp.float32(tokens * n_ctx))
    own, other = sides
    most = chips * tokens - half
    last = moving[1]
    handed = tdot(other[:most], every[:most])
    kept = tdot(own[:most], every[:most])
    handed, kept = lax.optimization_barrier((handed, kept))
    handed = (handed + tdot(other[most:], last)).astype(jnp.bfloat16)
    handed = lax.ppermute(handed, "ctx", swap)
    kept = lax.optimization_barrier(kept + tdot(own[most:], last))
    grad_weight = (kept + handed.astype(jnp.float32)) * scale
    return (grad_input, grad_weight)


def solution(mesh):
    placed = (P(("ctx", "tp"), None), P(("ctx", "tp"), None), P(None, "tp"), P("ctx", "tp"))

    return jax.shard_map(
        body,
        mesh=mesh,
        in_specs=placed,
        out_specs=(P(("ctx", "tp"), None), P("ctx", "tp")),
        check_vma=False,
    )
```

```python
import functools

import jax
import jax.numpy as jnp
from jax import lax
from jax.experimental import pallas as pl
from jax.experimental.pallas import tpu as pltpu
from jax.sharding import PartitionSpec as P

VMEM = pl.BlockSpec(memory_space=pltpu.VMEM)


def ring_order(length):
    return list(range(0, length, 2)) + list(range(length - 1 - (length % 2), 0, -2))


def prepare_kernel(order, block, codes_ref, exps_ref, *out_refs):
    chips = len(order)
    wide = out_refs[0].shape[-1]
    per = wide // block
    chip = lax.axis_index("ctx") // 2
    exps = exps_ref[...].astype(jnp.float32).T
    for step, out_ref in enumerate(out_refs):
        dest = jnp.int32(0)
        for i in range(chips):
            dest = dest + jnp.where(chip == order[i], order[(i + step) % chips], 0)
        chosen = jnp.zeros((exps.shape[0], per), jnp.float32)
        for k in range(chips):
            chosen = jnp.where(dest == k, exps[:, per * k : per * (k + 1)], chosen)
        scales = jnp.exp2(chosen)
        for j in range(per):
            column = pl.multiple_of(dest * wide + j * block, block)
            codes = codes_ref[:, pl.ds(column, block)].astype(jnp.float32)
            out_ref[:, j * block : (j + 1) * block] = (codes * scales[:, j : j + 1]).astype(
                jnp.bfloat16
            )


def prepare(codes, exponents, order):
    rows, width = codes.shape
    chips = len(order)
    out = jax.ShapeDtypeStruct((rows, width // chips), jnp.bfloat16)
    return pl.pallas_call(
        functools.partial(prepare_kernel, order, width // exponents.shape[1]),
        out_shape=[out] * chips,
        in_specs=[VMEM] * 2,
        out_specs=[VMEM] * chips,
        cost_estimate=pl.CostEstimate(
            flops=2 * rows * width, bytes_accessed=4 * rows * width, transcendentals=0
        ),
    )(codes, exponents.T)


def tdot(a, b):
    return lax.dot_general(a, b, (((0,), (0,)), ((), ())), preferred_element_type=jnp.float32)


def added(terms):
    return sum(t.astype(jnp.float32) for t in terms).astype(jnp.bfloat16)


def body(act_codes, scale_exps, weight, grad_out):
    width = act_codes.shape[1]
    n_ctx, n_tp = lax.axis_size("ctx"), lax.axis_size("tp")
    chips = n_ctx // 2
    tp = lax.axis_index("tp")
    rows = act_codes.shape[0]
    tokens = grad_out.shape[0]
    out_rows = width // n_ctx
    core = lax.axis_index("ctx") % 2
    order = ring_order(chips)
    half = tokens // 2

    swap = [(i, i ^ 1) for i in range(n_ctx)]

    def shift(step):
        return [
            (2 * order[i] + c, 2 * order[(i + step) % chips] + c)
            for i in range(chips)
            for c in range(2)
        ]

    def peers(j):
        return [(i, i ^ j) for i in range(n_tp)]

    every = jnp.zeros((chips * tokens, grad_out.shape[1]), jnp.bfloat16)
    every = lax.dynamic_update_slice(every, grad_out, (0, 0))
    moving = lax.ppermute(grad_out, "ctx", shift(1))
    every = lax.dynamic_update_slice(every, moving, (tokens, 0))
    moving = [moving[:half], moving[half:]]
    for step in range(2, chips):
        for h in range(2):
            moving[h] = lax.ppermute(moving[h], "ctx", shift(1))
            if step < chips - 1 or h == 0:
                every = lax.dynamic_update_slice(every, moving[h], (step * tokens + h * half, 0))

    pieces = list(prepare(act_codes, scale_exps, order))
    for step in range(1, chips):
        pieces[step] = lax.ppermute(pieces[step], "ctx", shift(step))
    pieces = jnp.stack(pieces)
    got = {0: pieces}
    if n_tp == 4:
        for j in (1, 2):
            got[j] = lax.ppermute(pieces, "tp", peers(j))
        middle = chips // 2
        first = lax.ppermute(got[1][:middle], "tp", peers(2))
        second = lax.ppermute(got[2][middle:], "tp", peers(1))
    else:
        for j in range(1, n_tp):
            got[j] = lax.ppermute(pieces, "tp", peers(j))
    if n_tp == 4:
        got[3] = None
    sides = []
    for side in range(2):
        acts = jnp.zeros((chips, n_tp, rows, out_rows), jnp.bfloat16)
        for j, part in got.items():
            blocks = [(0, part)] if part is not None else [(0, first), (middle, second)]
            for at, block in blocks:
                block = jnp.where(core == side, block[..., :out_rows], block[..., out_rows:])
                acts = lax.dynamic_update_slice(acts, block[:, None], (at, tp ^ j, 0, 0))
        sides.append(acts.reshape(chips * tokens, out_rows))

    outs = []
    span = width // 2
    bits = [1 << b for b in range(n_tp.bit_length() - 1)]
    for h in range(2):
        part = lax.dot_general(
            grad_out,
            lax.slice_in_dim(weight, h * span, (h + 1) * span),
            (((1,), (1,)), ((), ())),
            preferred_element_type=jnp.float32,
        ).astype(jnp.bfloat16)
        held = {j: [lax.dynamic_slice_in_dim(part, (tp ^ j) * rows, rows, 0)] for j in range(n_tp)}
        for bit in bits if h == 0 else bits[::-1]:
            leaving = [j for j in held if j & bit]
            sent = jnp.stack([added(held.pop(j)) for j in leaving])
            sent = lax.ppermute(sent, "tp", peers(bit))
            for i, j in enumerate(leaving):
                held[j ^ bit].append(sent[i])
        outs.append(added(held[0]))
    grad_input = jnp.concatenate(outs, axis=1)

    scale = lax.rsqrt(jnp.float32(tokens * n_ctx))
    own, other = sides
    most = chips * tokens - half
    last = moving[1]
    theirs = lax.ppermute(other[most:], "ctx", swap)
    handed = tdot(other[:most], every[:most]).astype(jnp.bfloat16)
    moved = lax.ppermute(handed, "ctx", swap)
    own, handed = lax.optimization_barrier((own, handed))
    kept = tdot(own[:most], every[:most])
    kept = lax.optimization_barrier(kept)
    swapped = lax.ppermute(last, "ctx", swap)
    kept = kept + moved.astype(jnp.float32) + tdot(own[most:], last)
    kept = lax.optimization_barrier(kept)
    grad_weight = (kept + tdot(theirs, swapped)) * scale
    return (grad_input, grad_weight)


def solution(mesh):
    placed = (P(("ctx", "tp"), None), P(("ctx", "tp"), None), P(None, "tp"), P("ctx", "tp"))

    return jax.shard_map(
        body,
        mesh=mesh,
        in_specs=placed,
        out_specs=(P(("ctx", "tp"), None), P("ctx", "tp")),
        check_vma=False,
    )
```

```python
import functools

import jax
import jax.numpy as jnp
from jax import lax
from jax.experimental import pallas as pl
from jax.experimental.pallas import tpu as pltpu
from jax.sharding import PartitionSpec as P

VMEM = pl.BlockSpec(memory_space=pltpu.VMEM)


def ring_order(length):
    return list(range(0, length, 2)) + list(range(length - 1 - (length % 2), 0, -2))


def prepare_kernel(order, block, codes_ref, exps_ref, *out_refs):
    chips = len(order)
    wide = out_refs[0].shape[-1]
    per = wide // block
    chip = lax.axis_index("ctx") // 2
    exps = exps_ref[...].astype(jnp.float32).T
    for step, out_ref in enumerate(out_refs):
        dest = jnp.int32(0)
        for i in range(chips):
            dest = dest + jnp.where(chip == order[i], order[(i + step) % chips], 0)
        chosen = jnp.zeros((exps.shape[0], per), jnp.float32)
        for k in range(chips):
            chosen = jnp.where(dest == k, exps[:, per * k : per * (k + 1)], chosen)
        scales = jnp.exp2(chosen)
        for j in range(per):
            column = pl.multiple_of(dest * wide + j * block, block)
            codes = codes_ref[:, pl.ds(column, block)].astype(jnp.float32)
            out_ref[:, j * block : (j + 1) * block] = (codes * scales[:, j : j + 1]).astype(
                jnp.bfloat16
            )


def prepare(codes, exponents, order):
    rows, width = codes.shape
    chips = len(order)
    out = jax.ShapeDtypeStruct((rows, width // chips), jnp.bfloat16)
    return pl.pallas_call(
        functools.partial(prepare_kernel, order, width // exponents.shape[1]),
        out_shape=[out] * chips,
        in_specs=[VMEM] * 2,
        out_specs=[VMEM] * chips,
        cost_estimate=pl.CostEstimate(
            flops=2 * rows * width, bytes_accessed=4 * rows * width, transcendentals=0
        ),
    )(codes, exponents.T)


def finish_kernel(count, at, part_ref, more_ref, *refs):
    out_ref, ready_ref, sems = refs[-3:]
    wide = part_ref.shape[1]
    step = wide // sems.shape[0]
    scale = lax.rsqrt(jnp.full((1, step), count, jnp.float32))
    copies = []
    for n in range(sems.shape[0]):
        cut = slice(n * step, (n + 1) * step)
        if len(refs) == 3:
            more = more_ref[:, cut].astype(jnp.float32)
        else:
            more = tdot(more_ref[...], refs[0][:, cut])
        ready_ref[:, cut] = (part_ref[:, cut] + more) * scale
        place = out_ref.at[:, at * wide + n * step : at * wide + (n + 1) * step]
        copies.append(pltpu.make_async_copy(ready_ref.at[:, cut], place, sems.at[n]))
        copies[-1].start()
    for copy in copies:
        copy.wait()


def finish(part, more, swapped, before, count, columns):
    rows, wide = part.shape
    if wide % 128:
        more = more.astype(jnp.float32) if swapped is None else tdot(more, swapped)
        part = (part + more) * lax.rsqrt(jnp.float32(count))
        return part if before is None else jnp.concatenate([before, part], axis=1)
    at = 0 if before is None else 1
    operands = [part, more] + ([] if before is None else [swapped, before])
    specs = [VMEM] * min(3, len(operands))
    if before is not None:
        specs.append(pl.BlockSpec(memory_space=pl.ANY))
    return pl.pallas_call(
        functools.partial(finish_kernel, count, at),
        out_shape=jax.ShapeDtypeStruct((rows, columns), jnp.float32),
        in_specs=specs,
        out_specs=pl.BlockSpec(memory_space=pl.ANY),
        scratch_shapes=[
            pltpu.VMEM((rows, wide), jnp.float32),
            pltpu.SemaphoreType.DMA((wide // 128 // (2 - wide // 128 % 2),)),
        ],
        input_output_aliases={} if before is None else {3: 0},
        compiler_params=pltpu.CompilerParams(vmem_limit_bytes=8 << 20),
        cost_estimate=pl.CostEstimate(
            flops=2 * rows * wide * 256, bytes_accessed=4 * rows * wide, transcendentals=0
        ),
    )(*operands)


def tdot(a, b):
    return lax.dot_general(a, b, (((0,), (0,)), ((), ())), preferred_element_type=jnp.float32)


def added(terms):
    return sum(t.astype(jnp.float32) for t in terms).astype(jnp.bfloat16)


def body(act_codes, scale_exps, weight, grad_out):
    width = act_codes.shape[1]
    n_ctx, n_tp = lax.axis_size("ctx"), lax.axis_size("tp")
    chips = n_ctx // 2
    tp = lax.axis_index("tp")
    rows = act_codes.shape[0]
    tokens = grad_out.shape[0]
    out_rows = width // n_ctx
    core = lax.axis_index("ctx") % 2
    order = ring_order(chips)

    swap = [(i, i ^ 1) for i in range(n_ctx)]

    def shift(step):
        return [
            (2 * order[i] + c, 2 * order[(i + step) % chips] + c)
            for i in range(chips)
            for c in range(2)
        ]

    def peers(j):
        return [(i, i ^ j) for i in range(n_tp)]

    columns = grad_out.shape[1]
    ends = (0, columns // 2, columns)
    every = []
    for h in range(2):
        size = (chips - h) * tokens
        block = jnp.zeros((size, ends[h + 1] - ends[h]), jnp.bfloat16)
        every.append(lax.dynamic_update_slice(block, grad_out[:, ends[h] : ends[h + 1]], (0, 0)))
    moving = lax.ppermute(grad_out, "ctx", shift(1))
    moving = [moving[:, ends[h] : ends[h + 1]] for h in range(2)]
    for h in range(2):
        every[h] = lax.dynamic_update_slice(every[h], moving[h], (tokens, 0))
    for step in range(2, chips):
        for h in range(2):
            moving[h] = lax.ppermute(moving[h], "ctx", shift(1))
            if step < chips - 1 or h == 0:
                every[h] = lax.dynamic_update_slice(every[h], moving[h], (step * tokens, 0))

    pieces = list(prepare(act_codes, scale_exps, order))
    for step in range(1, chips):
        pieces[step] = lax.ppermute(pieces[step], "ctx", shift(step))
    pieces = jnp.stack(pieces)
    got = {0: pieces}
    if n_tp == 4:
        for j in (1, 2):
            got[j] = lax.ppermute(pieces, "tp", peers(j))
        middle = chips // 2
        first = lax.ppermute(got[1][:middle], "tp", peers(2))
        second = lax.ppermute(got[2][middle:], "tp", peers(1))
    else:
        for j in range(1, n_tp):
            got[j] = lax.ppermute(pieces, "tp", peers(j))
    if n_tp == 4:
        got[3] = None
    sides = []
    for side in range(2):
        acts = jnp.zeros((chips, n_tp, rows, out_rows), jnp.bfloat16)
        for j, part in got.items():
            blocks = [(0, part)] if part is not None else [(0, first), (middle, second)]
            for at, block in blocks:
                block = jnp.where(core == side, block[..., :out_rows], block[..., out_rows:])
                acts = lax.dynamic_update_slice(acts, block[:, None], (at, tp ^ j, 0, 0))
        sides.append(acts.reshape(chips * tokens, out_rows))

    outs = []
    span = width // 2
    bits = [1 << b for b in range(n_tp.bit_length() - 1)]
    for h in range(2):
        part = lax.dot_general(
            grad_out,
            lax.slice_in_dim(weight, h * span, (h + 1) * span),
            (((1,), (1,)), ((), ())),
            preferred_element_type=jnp.float32,
        ).astype(jnp.bfloat16)
        held = {j: [lax.dynamic_slice_in_dim(part, (tp ^ j) * rows, rows, 0)] for j in range(n_tp)}
        for bit in bits if h == 0 else bits[::-1]:
            leaving = [j for j in held if j & bit]
            sent = jnp.stack([added(held.pop(j)) for j in leaving])
            sent = lax.ppermute(sent, "tp", peers(bit))
            for i, j in enumerate(leaving):
                held[j ^ bit].append(sent[i])
        outs.append(added(held[0]))
    grad_input = jnp.concatenate(outs, axis=1)

    scale_of = tokens * n_ctx
    own, other = sides
    most = (chips - 1) * tokens
    last = moving[1]
    theirs = lax.ppermute(other[most:], "ctx", swap)
    handed, kept = [], []
    for h, depth in enumerate((chips * tokens, most)):
        product = tdot(other[:depth], every[h]).astype(jnp.bfloat16)
        handed.append(lax.ppermute(product, "ctx", swap))
    for h, depth in enumerate((chips * tokens, most)):
        kept.append(lax.optimization_barrier(tdot(own[:depth], every[h])))
    grad_weight = finish(kept[0], handed[0], None, None, scale_of, columns)
    swapped = lax.ppermute(last, "ctx", swap)
    rest = kept[1] + handed[1].astype(jnp.float32) + tdot(own[most:], last)
    grad_weight = finish(rest, theirs, swapped, grad_weight, scale_of, columns)
    return (grad_input, grad_weight)


def solution(mesh):
    placed = (P(("ctx", "tp"), None), P(("ctx", "tp"), None), P(None, "tp"), P("ctx", "tp"))

    return jax.shard_map(
        body,
        mesh=mesh,
        in_specs=placed,
        out_specs=(P(("ctx", "tp"), None), P("ctx", "tp")),
        check_vma=False,
    )
```

```python
import functools

import jax
import jax.numpy as jnp
from jax import lax
from jax.experimental import pallas as pl
from jax.experimental.pallas import tpu as pltpu
from jax.sharding import PartitionSpec as P

VMEM = pl.BlockSpec(memory_space=pltpu.VMEM)


def ring_order(length):
    return list(range(0, length, 2)) + list(range(length - 1 - (length % 2), 0, -2))


def prepare_kernel(order, block, codes_ref, exps_ref, *out_refs):
    chips = len(order)
    wide = out_refs[0].shape[-1]
    per = wide // block
    chip = lax.axis_index("ctx") // 2
    exps = exps_ref[...].astype(jnp.float32).T
    for step, out_ref in enumerate(out_refs):
        dest = jnp.int32(0)
        for i in range(chips):
            dest = dest + jnp.where(chip == order[i], order[(i + step) % chips], 0)
        chosen = jnp.zeros((exps.shape[0], per), jnp.float32)
        for k in range(chips):
            chosen = jnp.where(dest == k, exps[:, per * k : per * (k + 1)], chosen)
        scales = jnp.exp2(chosen)
        for j in range(per):
            column = pl.multiple_of(dest * wide + j * block, block)
            codes = codes_ref[:, pl.ds(column, block)].astype(jnp.float32)
            out_ref[:, j * block : (j + 1) * block] = (codes * scales[:, j : j + 1]).astype(
                jnp.bfloat16
            )


def prepare(codes, exponents, order):
    rows, width = codes.shape
    chips = len(order)
    out = jax.ShapeDtypeStruct((rows, width // chips), jnp.bfloat16)
    return pl.pallas_call(
        functools.partial(prepare_kernel, order, width // exponents.shape[1]),
        out_shape=[out] * chips,
        in_specs=[VMEM] * 2,
        out_specs=[VMEM] * chips,
        cost_estimate=pl.CostEstimate(
            flops=2 * rows * width, bytes_accessed=4 * rows * width, transcendentals=0
        ),
    )(codes, exponents.T)


def finish_kernel(count, at, part_ref, more_ref, *refs):
    out_ref, ready_ref, sems = refs[-3:]
    wide = part_ref.shape[1]
    step = wide // sems.shape[0]
    scale = lax.rsqrt(jnp.full((1, step), count, jnp.float32))
    copies = []
    for n in range(sems.shape[0]):
        cut = slice(n * step, (n + 1) * step)
        if len(refs) == 3:
            more = more_ref[:, cut].astype(jnp.float32)
        else:
            more = tdot(more_ref[...], refs[0][:, cut])
        ready_ref[:, cut] = (part_ref[:, cut] + more) * scale
        place = out_ref.at[:, at * wide + n * step : at * wide + (n + 1) * step]
        copies.append(pltpu.make_async_copy(ready_ref.at[:, cut], place, sems.at[n]))
        copies[-1].start()
    for copy in copies:
        copy.wait()


def finish(part, more, swapped, before, count, columns):
    rows, wide = part.shape
    if wide % 128:
        more = more.astype(jnp.float32) if swapped is None else tdot(more, swapped)
        part = (part + more) * lax.rsqrt(jnp.float32(count))
        return part if before is None else jnp.concatenate([before, part], axis=1)
    at = 0 if before is None else 1
    operands = [part, more] + ([] if before is None else [swapped, before])
    specs = [VMEM] * min(3, len(operands))
    if before is not None:
        specs.append(pl.BlockSpec(memory_space=pl.ANY))
    return pl.pallas_call(
        functools.partial(finish_kernel, count, at),
        out_shape=jax.ShapeDtypeStruct((rows, columns), jnp.float32),
        in_specs=specs,
        out_specs=pl.BlockSpec(memory_space=pl.ANY),
        scratch_shapes=[
            pltpu.VMEM((rows, wide), jnp.float32),
            pltpu.SemaphoreType.DMA((wide // 128 // (2 - wide // 128 % 2),)),
        ],
        input_output_aliases={} if before is None else {3: 0},
        compiler_params=pltpu.CompilerParams(vmem_limit_bytes=8 << 20),
        cost_estimate=pl.CostEstimate(
            flops=2 * rows * wide * 256, bytes_accessed=4 * rows * wide, transcendentals=0
        ),
    )(*operands)


def tdot(a, b):
    return lax.dot_general(a, b, (((0,), (0,)), ((), ())), preferred_element_type=jnp.float32)


def added(terms):
    return sum(t.astype(jnp.float32) for t in terms).astype(jnp.bfloat16)


def body(act_codes, scale_exps, weight, grad_out):
    width = act_codes.shape[1]
    n_ctx, n_tp = lax.axis_size("ctx"), lax.axis_size("tp")
    chips = n_ctx // 2
    tp = lax.axis_index("tp")
    rows = act_codes.shape[0]
    tokens = grad_out.shape[0]
    out_rows = width // n_ctx
    core = lax.axis_index("ctx") % 2
    chip = lax.axis_index("ctx") // 2
    order = ring_order(chips)

    swap = [(i, i ^ 1) for i in range(n_ctx)]

    def shift(step):
        return [
            (2 * order[i] + c, 2 * order[(i + step) % chips] + c)
            for i in range(chips)
            for c in range(2)
        ]

    def peers(j):
        return [(i, i ^ j) for i in range(n_tp)]

    columns = grad_out.shape[1]
    ends = (0, columns // 2, columns)
    every = []
    for h in range(2):
        size = (chips - h) * tokens
        block = jnp.zeros((size, ends[h + 1] - ends[h]), jnp.bfloat16)
        every.append(lax.dynamic_update_slice(block, grad_out[:, ends[h] : ends[h + 1]], (0, 0)))
    moving = lax.ppermute(grad_out, "ctx", shift(1))
    moving = [moving[:, ends[h] : ends[h + 1]] for h in range(2)]
    for h in range(2):
        every[h] = lax.dynamic_update_slice(every[h], moving[h], (tokens, 0))
    fresh = [grad_out[:, ends[h] : ends[h + 1]] for h in range(2)]
    fresh = lax.optimization_barrier(tuple(fresh))
    inner = (chip > 0) & (chip < chips - 1)
    for step in range(2, chips):
        for h in range(2):
            pairs = shift(1)
            if chips == 4 and step == 3:
                moving[h] = jnp.where(inner, moving[h], fresh[h])
                pairs = [(i, i ^ 2) for i in range(n_ctx)]
            moving[h] = lax.ppermute(moving[h], "ctx", pairs)
            if step < chips - 1 or h == 0:
                every[h] = lax.dynamic_update_slice(every[h], moving[h], (step * tokens, 0))

    pieces = list(prepare(act_codes, scale_exps, order))
    for step in range(1, chips):
        pieces[step] = lax.ppermute(pieces[step], "ctx", shift(step))
    pieces = jnp.stack(pieces)
    got = {0: pieces}
    if n_tp == 4:
        for j in (1, 2):
            got[j] = lax.ppermute(pieces, "tp", peers(j))
        middle = chips // 2
        first = lax.ppermute(got[1][:middle], "tp", peers(2))
        second = lax.ppermute(got[2][middle:], "tp", peers(1))
    else:
        for j in range(1, n_tp):
            got[j] = lax.ppermute(pieces, "tp", peers(j))
    if n_tp == 4:
        got[3] = None
    sides = []
    for side in range(2):
        acts = jnp.zeros((chips, n_tp, rows, out_rows), jnp.bfloat16)
        for j, part in got.items():
            blocks = [(0, part)] if part is not None else [(0, first), (middle, second)]
            for at, block in blocks:
                block = jnp.where(core == side, block[..., :out_rows], block[..., out_rows:])
                acts = lax.dynamic_update_slice(acts, block[:, None], (at, tp ^ j, 0, 0))
        sides.append(acts.reshape(chips * tokens, out_rows))

    outs = []
    span = width // 2
    bits = [1 << b for b in range(n_tp.bit_length() - 1)]
    for h in range(2):
        part = lax.dot_general(
            grad_out,
            lax.slice_in_dim(weight, h * span, (h + 1) * span),
            (((1,), (1,)), ((), ())),
            preferred_element_type=jnp.float32,
        ).astype(jnp.bfloat16)
        held = {j: [lax.dynamic_slice_in_dim(part, (tp ^ j) * rows, rows, 0)] for j in range(n_tp)}
        for bit in bits if h == 0 else bits[::-1]:
            leaving = [j for j in held if j & bit]
            sent = jnp.stack([added(held.pop(j)) for j in leaving])
            sent = lax.ppermute(sent, "tp", peers(bit))
            for i, j in enumerate(leaving):
                held[j ^ bit].append(sent[i])
        outs.append(added(held[0]))
    grad_input = jnp.concatenate(outs, axis=1)

    scale_of = tokens * n_ctx
    own, other = sides
    most = (chips - 1) * tokens
    last = moving[1]
    theirs = lax.ppermute(other[most:], "ctx", swap)
    handed, kept = [], []
    for h, depth in enumerate((chips * tokens, most)):
        product = tdot(other[:depth], every[h]).astype(jnp.bfloat16)
        handed.append(lax.ppermute(product, "ctx", swap))
    for h, depth in enumerate((chips * tokens, most)):
        kept.append(lax.optimization_barrier(tdot(own[:depth], every[h])))
    grad_weight = finish(kept[0], handed[0], None, None, scale_of, columns)
    swapped = lax.ppermute(last, "ctx", swap)
    rest = kept[1] + handed[1].astype(jnp.float32) + tdot(own[most:], last)
    grad_weight = finish(rest, theirs, swapped, grad_weight, scale_of, columns)
    return (grad_input, grad_weight)


def solution(mesh):
    placed = (P(("ctx", "tp"), None), P(("ctx", "tp"), None), P(None, "tp"), P("ctx", "tp"))

    return jax.shard_map(
        body,
        mesh=mesh,
        in_specs=placed,
        out_specs=(P(("ctx", "tp"), None), P("ctx", "tp")),
        check_vma=False,
    )
```
